32 devices in a mesh: parts: 2 (over x), rows: 16 (over z, y, core).
Axes of the slice: x: 2, y: 2, z: 4, core: 2. Of those that a mesh axis runs over, the one named last changes fastest.
Arguments:
- feature_bin: int32 [16384, 700], P(('parts', 'rows')), parts along dimension 0, may hold values from 0 to 255
- doc_leaf: int32 [16384], P(('parts', 'rows')), parts along dimension 0, may hold values from 0 to 31
- current_score: float32 [16384], P(('parts', 'rows')), parts along dimension 0, may hold values from -8 to 8
- relevance: int32 [16384], P(('parts', 'rows')), parts along dimension 0, may hold values from 0 to 4
- doc_rank: int32 [16384], P(('parts', 'rows')), parts along dimension 0, may hold values from 0 to 255, as said below
- query_length: int32 [64], P(('parts', 'rows')), parts along dimension 0, may hold values from 10 to 256, as said below
- feature_votes: int32 [32, 32, 20], P(('parts', 'rows')), parts along dimension 0, may hold values from 0 to 699, all different within a row
- elected: int32 [64, 40], P('parts'), parts along dimension 0, may hold values from 0 to 699, all different within a row
Outputs:
- gradient: float32 [16384], P(('parts', 'rows')), parts along dimension 0
- hessian: float32 [16384], P(('parts', 'rows')), parts along dimension 0
- vote_count: int32 [64, 700], P('parts'), parts along dimension 0
- split_gain: float32 [64, 40, 256], P('parts'), parts along dimension 0
The draws below stay inside these ranges and needn't reach their ends.
There are 2 independent parts, one for each index of `parts`. The reference program is written for one: setup_inputs(seed, part) draws one part's arguments, and reference() takes and returns one part's arrays. A program takes and returns all parts, laid end to end along the dimension named above; each array names one. Nothing has to cross between parts.
Inputs may be any that keep to these rules, and one draw needn't show every extreme that they name: `query_length`: query q holds slots q * 256 to (q + 1) * 256 - 1 of the document arrays; in every draw some query has exactly 256 documents. `doc_rank`: within each query the live documents hold positions 0 to query_length - 1, each once; slots that are not live hold positions from query_length to 255. `feature_votes`: the 20 votes of one device for one leaf are different features. The 40 elected features of one leaf are different.
All inputs are finite; a program needn't handle non-finite values.
Results may differ from the reference program's by a relative error of at most 0.0003.
Values sent between devices are 32-bit elements; how exact they have to be, the bound alone decides.
A program may use at most 64 MiB of HBM per device.

```python
import jax
import jax.numpy as jnp
from jax import lax

F = 700
B = 256
K = 20
E = 40
LEAVES = 32
QMAX = 256
QDEV = 2
NQ = 32
DOCS = 8192
N_ROWS = 16


def shared_lengths(key):
    base = jax.random.fold_in(key, 11)
    first, second, third = jax.random.split(base, 3)
    devices = NQ // QDEV
    limits = jax.random.randint(first, (devices, 1), QMAX // 4, QMAX - 9)
    extras = jax.random.randint(second, (devices, QDEV), 0, QMAX - 9)
    lengths = (10 + extras % (limits + 1)).reshape(-1)
    longest = jax.random.randint(third, (), 0, NQ)
    lengths = jnp.where(jnp.arange(NQ, dtype=jnp.int32) == longest, QMAX, lengths)
    return lengths.astype(jnp.int32)


def draw_query_length(key, part):
    return shared_lengths(key)


def draw_doc_rank(key, part):
    lengths = shared_lengths(key)
    keys = jax.random.split(jax.random.fold_in(key, 23), NQ)
    orders = jax.vmap(lambda single: jax.random.permutation(single, QMAX))(keys).astype(jnp.int32)
    living = jnp.arange(QMAX, dtype=jnp.int32)[None, :] < lengths[:, None]
    sorting = jnp.where(living, orders, orders + QMAX)
    places = jnp.argsort(jnp.argsort(sorting, axis=1), axis=1)
    return places.reshape(-1).astype(jnp.int32)


def place_ends(drawn, stream_key, least, top_value):
    place = [jax.random.randint(jax.random.fold_in(stream_key, axis), (), 0, length) for axis, length in enumerate(drawn.shape)]
    main_axis = drawn.shape.index(max(drawn.shape))
    neighbour = place[:main_axis] + [(place[main_axis] + 1) % drawn.shape[main_axis]] + place[main_axis + 1:]
    return drawn.at[tuple(place)].set(least).at[tuple(neighbour)].set(top_value)


def level_of(stream_key, extent, pieces, low, high):
    gain = 1.0
    for position, blocks in pieces:
        heights = jax.random.uniform(jax.random.fold_in(jax.random.fold_in(stream_key, 6), position), (blocks,), jnp.float32, low / len(pieces), high / len(pieces))
        gain = gain * jnp.repeat(jnp.exp(heights), extent[position] // blocks).reshape((-1,) + (1,) * (len(extent) - 1 - position))
    return gain


def different_ones(key, rows, count, top, lift):
    order = jax.random.permutation(jax.random.fold_in(key, 1), count)
    pull = order
    for power in range(3):
        pull = pull * pull // count
    pull = pull * lift // count
    lots = jax.random.randint(jax.random.fold_in(key, 2), (rows, count), 0, 4096) + pull
    holders = jax.random.permutation(jax.random.fold_in(key, 3), rows)[jnp.arange(count) % rows]
    lots = jnp.where(jnp.arange(rows)[:, None] == holders[None, :], 1 << 14, lots)
    merit = lots * count + jnp.arange(count)
    return lax.top_k(merit.astype(jnp.int32), top)[1].astype(jnp.int32)


def noise(own_key, dims, width, limit, pieces=(), kind=jnp.bfloat16):
    entries = jax.random.normal(own_key, dims, jnp.float32) * width
    if len(pieces) > 0:
        entries = level_of(own_key, dims, pieces, -0.22, 0.18) * entries
    return jnp.clip(entries, min=-limit, max=limit).astype(kind)


def setup_inputs(seed: int = 0, part: int = 0) -> dict:
    splits = jax.random.split(jax.random.key(seed), 9)
    part_splits = jax.random.split(jax.random.fold_in(splits[8], part), 9)
    feature_bin = place_ends(jax.random.randint(part_splits[0], (DOCS, F), 0, B), jax.random.fold_in(part_splits[0], 1), 0, B - 1).astype(jnp.int32)
    doc_leaf = place_ends(jax.random.randint(part_splits[1], (DOCS,), 0, LEAVES), jax.random.fold_in(part_splits[1], 1), 0, LEAVES - 1).astype(jnp.int32)
    current_score = noise(part_splits[2], (DOCS,), 2.0, 8.0, ((0, 16),), jnp.float32)
    relevance = place_ends(jax.random.randint(part_splits[3], (DOCS,), 0, 5), jax.random.fold_in(part_splits[3], 1), 0, 4).astype(jnp.int32)
    doc_rank = draw_doc_rank(jax.random.fold_in(jax.random.fold_in(splits[8], part), 71), part)
    query_length = draw_query_length(jax.random.fold_in(jax.random.fold_in(splits[8], part), 71), part)
    feature_votes = different_ones(part_splits[6], N_ROWS * LEAVES, F, K, 468).reshape((N_ROWS, LEAVES, K))
    elected = different_ones(part_splits[7], LEAVES, F, E, 0)
    return {"feature_bin": feature_bin, "doc_leaf": doc_leaf, "current_score": current_score, "relevance": relevance, "doc_rank": doc_rank, "query_length": query_length, "feature_votes": feature_votes, "elected": elected}


ridge_weight = 1.0


def query_terms(scores, levels, places, length):
    positions = jnp.arange(scores.shape[0], dtype=jnp.int32)
    living = positions < length
    gains = jnp.exp2(levels.astype(jnp.float32)) - 1.0
    discount = 1.0 / jnp.log2(places.astype(jnp.float32) + 2.0)
    higher = (levels[None, :] > levels[:, None]) & living[None, :]
    earlier = (levels[None, :] == levels[:, None]) & (positions[None, :] < positions[:, None]) & living[None, :]
    ideal_place = jnp.sum((higher | earlier).astype(jnp.float32), axis=1)
    ideal = jnp.sum(jnp.where(living, gains / jnp.log2(ideal_place + 2.0), 0.0))
    scaling = 1.0 / jnp.maximum(ideal, 1.0)
    ordered = (levels[:, None] > levels[None, :]) & living[:, None] & living[None, :]
    chance = jax.nn.sigmoid(scores[None, :] - scores[:, None])
    change = (gains[:, None] - gains[None, :]) * jnp.abs(discount[:, None] - discount[None, :]) * scaling
    pushes = jnp.where(ordered, chance * change, 0.0)
    curves = jnp.where(ordered, chance * (1.0 - chance) * change, 0.0)
    return jnp.sum(pushes, axis=0) - jnp.sum(pushes, axis=1), jnp.sum(curves, axis=0) + jnp.sum(curves, axis=1)


def build_histogram(feature_bin, doc_leaf, gradient, hessian, elected, bins):
    leaves, picked = elected.shape
    columns = elected[doc_leaf]
    chosen = jnp.take_along_axis(feature_bin, columns, axis=1)
    target = (doc_leaf[:, None] * picked + jnp.arange(picked, dtype=jnp.int32)[None, :]) * bins + chosen
    target = target.astype(jnp.int32).reshape(-1)
    segments = leaves * picked * bins
    grad_terms = jnp.broadcast_to(gradient[:, None], (gradient.shape[0], picked)).reshape(-1)
    hess_terms = jnp.broadcast_to(hessian[:, None], (hessian.shape[0], picked)).reshape(-1)
    grad_hist = jax.ops.segment_sum(grad_terms, target, segments)
    hess_hist = jax.ops.segment_sum(hess_terms, target, segments)
    return jnp.stack([grad_hist, hess_hist]).reshape(2, leaves, picked, bins)


def split_score(prefix, whole):
    remain = whole - prefix
    return (prefix[0] * prefix[0] / (prefix[1] + ridge_weight)
            + remain[0] * remain[0] / (remain[1] + ridge_weight)
            - whole[0] * whole[0] / (whole[1] + ridge_weight))


def count_votes(feature_votes, features):
    hits = feature_votes[..., None] == jnp.arange(features, dtype=jnp.int32)
    return jnp.sum(hits.astype(jnp.int32), axis=(0, 2)).astype(jnp.int32)


def reference(feature_bin, doc_leaf, current_score, relevance, doc_rank, query_length, feature_votes, elected):
    def one_query(items):
        return query_terms(items[0], items[1], items[2], items[3])

    gradient, hessian = lax.map(one_query, (current_score.reshape(-1, QMAX), relevance.reshape(-1, QMAX),
                                            doc_rank.reshape(-1, QMAX), query_length))
    gradient = gradient.reshape(-1)
    hessian = hessian.reshape(-1)
    vote_count = count_votes(feature_votes, F)
    histogram = build_histogram(feature_bin, doc_leaf, gradient, hessian, elected, B)
    prefix = jnp.cumsum(histogram, axis=3)
    whole = jnp.sum(histogram, axis=3, keepdims=True)
    split_gain = split_score(prefix, whole)
    return gradient, hessian, vote_count, split_gain
```

```python
import functools
import math

import jax
import jax.numpy as jnp
from jax import lax
from jax.experimental import pallas as pl
from jax.experimental.pallas import tpu as pltpu
from jax.sharding import PartitionSpec as P

B = 256
QMAX = 256
LANES = 128
TERMS = 3

ridge_weight = 1.0
F32 = jnp.float32
BF16 = jnp.bfloat16
NT = (((1,), (1,)), ((), ()))
VMEM = pl.BlockSpec(memory_space=pltpu.VMEM)


def slot_of(owner, turn, n):
    return turn * n + (owner % 2) * (n // 2) + owner // 2


def local_kernel(n, turns, fb_ref, leaf_ref, score_ref, rel_ref, rank_ref, qlen_ref, elected_ref,
                 votes_ref, send_ref, grad_ref, hess_ref, packed_ref, hot_ref, stack_ref, all_ref):
    docs, features = fb_ref.shape
    leaves, picked = elected_ref.shape
    chunks = docs // LANES
    per_query = QMAX // LANES

    groups = leaves // 8
    pitch = LANES // groups
    packed_ref[...] = jnp.full(packed_ref.shape, -1, jnp.int32)
    for g in range(groups):
        packed_ref[:, g * pitch:g * pitch + votes_ref.shape[2]] = votes_ref[0, g * 8:(g + 1) * 8, :]

    lanes = lax.broadcasted_iota(jnp.int32, (leaves, features), 1)
    for e in range(picked):
        hot_ref[e * leaves:(e + 1) * leaves, :] = jnp.where(
            elected_ref[:, e:e + 1] == lanes, 1.0, 0.0).astype(BF16)
    bins = fb_ref[...].astype(F32).astype(BF16)
    all_ref[...] = lax.dot_general(hot_ref[...], bins, NT, preferred_element_type=F32)

    rel = rel_ref[...].astype(F32)
    gain = jnp.exp2(rel) - 1.0
    disc = math.log(2.0) / jnp.log(rank_ref[...].astype(F32) + 2.0)
    row = lax.broadcasted_iota(jnp.int32, (chunks, LANES), 0)
    slot = (row % per_query) * LANES + lax.broadcasted_iota(jnp.int32, (chunks, LANES), 1)
    length = jnp.zeros((chunks, LANES), jnp.int32)
    for q in range(chunks // per_query):
        length = jnp.where(row // per_query == q, qlen_ref[q], length)
    live = slot < length
    livef = jnp.where(live, 1.0, 0.0)
    key = rel * float(QMAX) + (QMAX - 1 - slot).astype(F32)
    score = score_ref[...]
    stack_ref[...] = jnp.zeros(stack_ref.shape, F32)
    for index, item in enumerate((score, gain, disc, jnp.where(live, key, -1.0), livef)):
        stack_ref[index * chunks:(index + 1) * chunks, :] = item
    turned = stack_ref[...].T

    def column(index, c):
        return turned[:, index * chunks + c:index * chunks + c + 1]

    for q in range(chunks // per_query):
        mine = range(q * per_query, (q + 1) * per_query)
        ideal = jnp.zeros((1, 1), F32)
        sums = []
        for j in mine:
            srow, grow, drow, krow = score[j:j + 1], gain[j:j + 1], disc[j:j + 1], key[j:j + 1]
            place = jnp.zeros((1, LANES), F32)
            push = jnp.zeros((1, LANES), F32)
            curve = jnp.zeros((1, LANES), F32)
            for i in mine:
                place += jnp.sum(jnp.where(column(3, i) > krow, 1.0, 0.0), axis=0, keepdims=True)
                apart = column(0, i) - srow
                step = column(1, i) - grow
                chance = 1.0 / (1.0 + jnp.exp(jnp.where(step > 0.0, apart, -apart)))
                part = chance * jnp.abs(column(2, i) - drow) * column(4, i)
                signed = part * step
                push += jnp.sum(signed, axis=0, keepdims=True)
                curve += jnp.sum(jnp.abs(signed) * (1.0 - chance), axis=0, keepdims=True)
            top = livef[j:j + 1] * grow * (math.log(2.0) / jnp.log(place + 2.0))
            ideal += jnp.sum(top, axis=1, keepdims=True)
            sums.append((push, curve))
        scaling = 1.0 / jnp.maximum(ideal, 1.0)
        for j, (push, curve) in zip(mine, sums):
            grad_ref[j:j + 1, :] = push * livef[j:j + 1] * scaling
            hess_ref[j:j + 1, :] = curve * livef[j:j + 1] * scaling

    sub = lax.broadcasted_iota(jnp.int32, (leaves, LANES), 0)
    own = [leaf_ref[c:c + 1, :] == sub for c in range(chunks)]
    grad, hess, leaf = grad_ref[...], hess_ref[...], leaf_ref[...].astype(F32)
    for i in range(n):
        base = turns * chunks
        for turn in range(turns):
            e = slot_of(i, turn, n)
            if e < picked:
                for c in range(chunks):
                    block = all_ref[e * leaves:(e + 1) * leaves, c * LANES:(c + 1) * LANES]
                    send_ref[i, turn * chunks + c:turn * chunks + c + 1, :] = jnp.sum(
                        jnp.where(own[c], block, 0.0), axis=0, keepdims=True)
            else:
                send_ref[i, turn * chunks:(turn + 1) * chunks, :] = jnp.zeros((chunks, LANES), F32)
        send_ref[i, base:base + chunks, :] = grad
        send_ref[i, base + chunks:base + 2 * chunks, :] = hess
        send_ref[i, base + 2 * chunks:base + 3 * chunks, :] = leaf
        rest = send_ref.shape[1] - base - 3 * chunks
        if rest:
            send_ref[i, base + 3 * chunks:, :] = jnp.zeros((rest, LANES), F32)


def shared_kernel(n, turns, chunks, picked, votes_each, packed_ref, send_ref, count_ref, out_ref,
                  votes_ref, docs_ref, weight_ref, vs, vr, ds, dr, rs, rr, ls, lr, ss, sr):
    leaves, features = count_ref.shape
    chips = n // 2
    me = lax.axis_index("rows")
    core, chip = lax.rem(me, 2), me // 2

    def place_of(c):
        return jnp.where(c % 2 == 0, c // 2, chips - 1 - c // 2)

    def chip_at(p):
        return jnp.where(p < chips // 2, 2 * p, 2 * (chips - 1 - p) + 1)

    place = place_of(chip)

    def at(offset):
        return chip_at(lax.rem(place + offset + chips, chips)) * 2 + core

    sibling = me + 1 - 2 * core

    barrier = pltpu.get_barrier_semaphore()

    def greet(k, _):
        pl.semaphore_signal(barrier, inc=1, device_id={"rows": lax.rem(me + k, n)},
                            device_id_type=pl.DeviceIdType.MESH)
        return 0

    lax.fori_loop(1, n, greet, 0)
    pl.semaphore_wait(barrier, n - 1)

    def votes_copy(k):
        return pltpu.make_async_remote_copy(
            src_ref=packed_ref, dst_ref=votes_ref.at[me], send_sem=vs.at[k], recv_sem=vr.at[k],
            device_id={"rows": lax.rem(me + k, n)}, device_id_type=pl.DeviceIdType.MESH)

    def docs_copy(k):
        there = lax.rem(me + k, n)
        return pltpu.make_async_remote_copy(
            src_ref=send_ref.at[there], dst_ref=docs_ref.at[me], send_sem=ds.at[k],
            recv_sem=dr.at[k], device_id={"rows": there}, device_id_type=pl.DeviceIdType.MESH)

    def start_both(k, _):
        votes_copy(k).start()
        return 0

    def start_docs(k, _):
        docs_copy(k).start()
        return 0

    lax.fori_loop(1, n, start_both, 0)
    lax.fori_loop(1, n, start_docs, 0)
    votes_ref[me] = packed_ref[...]
    docs_ref[me] = send_ref[me]

    def wait_votes(k, _):
        votes_copy(k).wait()
        return 0

    lax.fori_loop(1, n, wait_votes, 0)
    groups = leaves // 8
    pitch = LANES // groups
    numbers = lax.broadcasted_iota(jnp.int32, (8, features), 1)

    def count(p, totals):
        tile = votes_ref[p]
        grown = []
        for g in range(groups):
            total = totals[g]
            for k in range(votes_each):
                total += jnp.where(tile[:, g * pitch + k:g * pitch + k + 1] == numbers, 1, 0)
            grown.append(total)
        return tuple(grown)

    totals = lax.fori_loop(0, n, count, (jnp.zeros((8, features), jnp.int32),) * groups)
    for g in range(groups):
        count_ref[g * 8:(g + 1) * 8, :] = totals[g]

    def wait_docs(k, _):
        docs_copy(k).wait()
        return 0

    lax.fori_loop(1, n, wait_docs, 0)
    sub = lax.broadcasted_iota(jnp.int32, (leaves, LANES), 0).astype(F32)
    base = turns * chunks

    def weigh(p, _):
        for c in range(chunks):
            own = docs_ref[p, base + 2 * chunks + c:base + 2 * chunks + c + 1, :] == sub
            for which in range(2):
                at_row = base + which * chunks + c
                left = docs_ref[p, at_row:at_row + 1, :]
                for term in range(TERMS):
                    piece = left.astype(BF16).astype(F32)
                    left = left - piece
                    at_weight = (term * 2 + which) * leaves
                    weight_ref[p, at_weight:at_weight + leaves, c * LANES:(c + 1) * LANES] = (
                        jnp.where(own, piece, 0.0).astype(BF16))
        return 0

    lax.fori_loop(0, n, weigh, 0)
    steps = lax.broadcasted_iota(jnp.int32, (B, LANES), 0).astype(F32)

    def tile_copy(slot, sems, rsems, index, there):
        return pltpu.make_async_remote_copy(
            src_ref=out_ref.at[slot], dst_ref=out_ref.at[slot], send_sem=sems.at[index],
            recv_sem=rsems.at[index], device_id={"rows": there},
            device_id_type=pl.DeviceIdType.MESH)

    far = chips // 2
    near = chips - 1 - far

    def right_copy(hop, turn):
        return tile_copy(slot_of(at(-hop), turn, n), rs, rr, hop * turns + turn, at(1))

    def left_copy(hop, turn):
        return tile_copy(slot_of(at(hop), turn, n), ls, lr, hop * turns + turn, at(-1))

    def sibling_copy(offset, turn):
        index = (offset + chips) % chips * turns + turn
        return tile_copy(slot_of(at(offset), turn, n), ss, sr, index, sibling)

    def exists(offset, turn):
        return slot_of(at(offset), turn, n) < picked

    def reach(hop, last_core):
        if hop <= near:
            return True
        if hop > far:
            return False
        return core == last_core

    def when(ok, also=True):
        if also is True:
            return pl.when(ok)
        return pl.when(jnp.logical_and(ok, also))

    for turn in range(turns):
        mine = slot_of(me, turn, n)

        @pl.when(mine < picked)
        def _(turn=turn, mine=mine):
            def add(p, total):
                tall = []
                for c in range(chunks):
                    bins = docs_ref[p, turn * chunks + c:turn * chunks + c + 1, :]
                    tall.append(jnp.where(bins <= steps, 1.0, 0.0).astype(BF16))
                return total + lax.dot_general(
                    weight_ref[p], jnp.concatenate(tall, axis=1), NT, preferred_element_type=F32)

            total = lax.fori_loop(0, n, add, jnp.zeros((TERMS * 2 * leaves, B), F32))
            both = total[:2 * leaves]
            for term in range(1, TERMS):
                both += total[term * 2 * leaves:(term + 1) * 2 * leaves]
            pg, ph = both[:leaves], both[leaves:]
            wg, wh = pg[:, B - 1:], ph[:, B - 1:]
            og, oh = wg - pg, wh - ph
            out_ref[mine] = (pg * pg / (ph + ridge_weight) + og * og / (oh + ridge_weight)
                             - wg * wg / (wh + ridge_weight))

        @pl.when(mine < picked)
        def _(turn=turn):
            right_copy(0, turn).start()
            left_copy(0, turn).start()
            sibling_copy(0, turn).start()

    for hop in range(1, far + 1):
        for turn in range(turns):
            arrives = reach(hop, 0)
            if arrives is not False:

                @when(exists(-hop, turn), arrives)
                def _(hop=hop, turn=turn):
                    tile_copy(slot_of(at(-hop), turn, n), rs, rr, (hop - 1) * turns + turn,
                              at(1)).wait_recv()
                    sibling_copy(-hop, turn).start()

                onward = reach(hop + 1, 0)
                if onward is not False:

                    @when(exists(-hop, turn), onward)
                    def _(hop=hop, turn=turn):
                        right_copy(hop, turn).start()

            arrives = reach(hop, 1)
            if arrives is not False:

                @when(exists(hop, turn), arrives)
                def _(hop=hop, turn=turn):
                    tile_copy(slot_of(at(hop), turn, n), ls, lr, (hop - 1) * turns + turn,
                              at(-1)).wait_recv()
                    sibling_copy(hop, turn).start()

                onward = reach(hop + 1, 1)
                if onward is not False:

                    @when(exists(hop, turn), onward)
                    def _(hop=hop, turn=turn):
                        left_copy(hop, turn).start()

    def other(offset, turn):
        return slot_of(at(offset) + 1 - 2 * core, turn, n)

    for turn in range(turns):
        for offset in range(chips):

            @pl.when(other(offset, turn) < picked)
            def _(offset=offset, turn=turn):
                tile_copy(other(offset, turn), ss, sr, offset * turns + turn, sibling).wait_recv()

            @pl.when(exists(offset, turn))
            def _(offset=offset, turn=turn):
                sibling_copy(offset, turn).wait_send()

        for hop in range(far):
            onward = reach(hop + 1, 0)
            if onward is not False:

                @when(exists(-hop, turn), onward)
                def _(hop=hop, turn=turn):
                    right_copy(hop, turn).wait_send()

            onward = reach(hop + 1, 1)
            if onward is not False:

                @when(exists(hop, turn), onward)
                def _(hop=hop, turn=turn):
                    left_copy(hop, turn).wait_send()


def on_device(n, feature_bin, doc_leaf, current_score, relevance, doc_rank, query_length,
              feature_votes, elected):
    docs, features = feature_bin.shape
    leaves, picked = elected.shape
    each = feature_votes.shape[2]
    turns = -(-picked // n)
    chunks = docs // LANES
    rows = -(-(turns + 3) * chunks // 8) * 8
    chips = n // 2
    far = chips // 2

    def lay(a):
        return a.reshape(chunks, LANES)

    send, gradient, hessian, packed = pl.pallas_call(
        functools.partial(local_kernel, n, turns),
        out_shape=(
            jax.ShapeDtypeStruct((n, rows, LANES), F32),
            jax.ShapeDtypeStruct((chunks, LANES), F32),
            jax.ShapeDtypeStruct((chunks, LANES), F32),
            jax.ShapeDtypeStruct((8, LANES), jnp.int32),
        ),
        in_specs=[VMEM] * 5 + [pl.BlockSpec(memory_space=pltpu.SMEM)] + [VMEM] * 2,
        out_specs=(VMEM,) * 4,
        scratch_shapes=[
            pltpu.VMEM((picked * leaves, features), BF16),
            pltpu.VMEM((LANES, LANES), F32),
            pltpu.VMEM((picked * leaves, docs), F32),
        ],
        compiler_params=pltpu.CompilerParams(vmem_limit_bytes=40 * 2**20),
        name="local",
    )(feature_bin, lay(doc_leaf), lay(current_score), lay(relevance), lay(doc_rank), query_length,
      elected, feature_votes)

    dma = pltpu.SemaphoreType.DMA
    vote_count, gathered = pl.pallas_call(
        functools.partial(shared_kernel, n, turns, chunks, picked, each),
        out_shape=(
            jax.ShapeDtypeStruct((leaves, features), jnp.int32),
            jax.ShapeDtypeStruct((picked, leaves, B), F32),
        ),
        in_specs=[VMEM] * 2,
        out_specs=(VMEM,) * 2,
        scratch_shapes=[
            pltpu.VMEM((n, 8, LANES), jnp.int32),
            pltpu.VMEM((n, rows, LANES), F32),
            pltpu.VMEM((n, TERMS * 2 * leaves, docs), BF16),
            dma((n,)), dma((n,)), dma((n,)), dma((n,)),
            dma((far * turns,)), dma((far * turns,)),
            dma((far * turns,)), dma((far * turns,)),
            dma((chips * turns,)), dma((chips * turns,)),
        ],
        compiler_params=pltpu.CompilerParams(
            collective_id=0, has_side_effects=True, vmem_limit_bytes=48 * 2**20),
        name="shared",
    )(packed, send)
    split_gain = jnp.transpose(gathered, (1, 0, 2))
    return gradient.reshape(-1), hessian.reshape(-1), vote_count, split_gain


def solution(mesh):
    n = mesh.shape["rows"]
    return jax.shard_map(
        functools.partial(on_device, n),
        mesh=mesh,
        in_specs=(
            P(("parts", "rows"), None),
            P(("parts", "rows")),
            P(("parts", "rows")),
            P(("parts", "rows")),
            P(("parts", "rows")),
            P(("parts", "rows")),
            P(("parts", "rows"), None, None),
            P("parts", None),
        ),
        out_specs=(
            P(("parts", "rows")),
            P(("parts", "rows")),
            P("parts", None),
            P("parts", None, None),
        ),
        check_vma=False,
    )
```

```python
import functools
import math

import jax
import jax.numpy as jnp
from jax import lax
from jax.experimental import pallas as pl
from jax.experimental.pallas import tpu as pltpu
from jax.sharding import PartitionSpec as P

B = 256
QMAX = 256
LANES = 128
SUB = 16
TERMS = 2
UNROLL = 4

ridge_weight = 1.0
F32 = jnp.float32
BF16 = jnp.bfloat16
NT = (((1,), (1,)), ((), ()))
NN = (((1,), (0,)), ((), ()))
VMEM = pl.BlockSpec(memory_space=pltpu.VMEM)
MESH = pl.DeviceIdType.MESH


def slot_of(owner, turn, n):
    return turn * n + (owner % 2) * (n // 2) + owner // 2


def pair_terms(chunks, leaf_ref, score_ref, rel_ref, rank_ref, qlen_ref, votes_ref, packed_ref,
               stack_ref, grad_ref, hess_ref, leaves):
    per_query = QMAX // LANES
    each = votes_ref.shape[0]
    rel = rel_ref[...].astype(F32)
    gain = jnp.exp2(rel) - 1.0
    disc = math.log(2.0) / jnp.log(rank_ref[...].astype(F32) + 2.0)
    row = lax.broadcasted_iota(jnp.int32, (chunks, LANES), 0)
    slot = (row % per_query) * LANES + lax.broadcasted_iota(jnp.int32, (chunks, LANES), 1)
    length = jnp.zeros((chunks, LANES), jnp.int32)
    for q in range(chunks // per_query):
        length = jnp.where(row // per_query == q, qlen_ref[q], length)
    live = slot < length
    livef = jnp.where(live, 1.0, 0.0)
    key = rel * float(QMAX) + (QMAX - 1 - slot).astype(F32)
    score = score_ref[...]
    stack_ref[...] = jnp.zeros(stack_ref.shape, F32)
    items = (score, gain, disc, jnp.where(live, key, -1.0), livef)
    for index, item in enumerate(items):
        stack_ref[index * chunks:(index + 1) * chunks, :] = item
    first = len(items) * chunks
    for k in range(each):
        stack_ref[first + k:first + k + 1, 0:leaves] = votes_ref[k].astype(F32)
    turned = stack_ref[...].T

    groups = leaves // 8
    pitch = LANES // groups
    packed_ref[...] = jnp.full(packed_ref.shape, -1, jnp.int32)
    for g in range(groups):
        packed_ref[:, g * pitch:g * pitch + each] = turned[
            g * 8:(g + 1) * 8, first:first + each].astype(jnp.int32)

    def column(index, c):
        return turned[:, index * chunks + c:index * chunks + c + 1]

    for q in range(chunks // per_query):
        mine = range(q * per_query, (q + 1) * per_query)
        ideal = jnp.zeros((1, 1), F32)
        sums = []
        for j in mine:
            srow, grow, drow, krow = score[j:j + 1], gain[j:j + 1], disc[j:j + 1], key[j:j + 1]
            place = jnp.zeros((1, LANES), F32)
            push = jnp.zeros((1, LANES), F32)
            curve = jnp.zeros((1, LANES), F32)
            for i in mine:
                place += jnp.sum(jnp.where(column(3, i) > krow, 1.0, 0.0), axis=0, keepdims=True)
                apart = column(0, i) - srow
                step = column(1, i) - grow
                chance = 1.0 / (1.0 + jnp.exp(jnp.where(step > 0.0, apart, -apart)))
                part = chance * jnp.abs(column(2, i) - drow) * column(4, i)
                signed = part * step
                push += jnp.sum(signed, axis=0, keepdims=True)
                curve += jnp.sum(jnp.abs(signed) * (1.0 - chance), axis=0, keepdims=True)
            top = livef[j:j + 1] * grow * (math.log(2.0) / jnp.log(place + 2.0))
            ideal += jnp.sum(top, axis=1, keepdims=True)
            sums.append((push, curve))
        scaling = 1.0 / jnp.maximum(ideal, 1.0)
        for j, (push, curve) in zip(mine, sums):
            grad_ref[j:j + 1, :] = push * livef[j:j + 1] * scaling
            hess_ref[j:j + 1, :] = curve * livef[j:j + 1] * scaling


def kernel(n, turns, fb_hbm, leaf_hbm, score_hbm, rel_hbm, rank_hbm, qlen_hbm, elected_hbm,
           votes_hbm, grad_ref, hess_ref, count_ref, gain_hbm,
           fb_ref, leaf_ref, score_ref, rel_ref, rank_ref, qlen_ref, elected_ref, votes_in,
           hot_ref, stack_ref, all_ref, packed_ref, send_ref,
           votes_ref, docs_ref, weight_ref, out_ref, load_sem, save_sem, vs, vr, ds, dr, zs, zr, ys, yr, ss, sr):
    features, docs = fb_ref.shape
    leaves, picked = elected_ref.shape
    votes_each = votes_in.shape[0]
    chunks = docs // LANES
    base = turns * chunks
    chips = n // 2
    lines = chips // 2
    me = lax.axis_index("rows")
    core, side, line = me % 2, (me // 2) % 2, me // 4

    def device(line_, side_, core_):
        return line_ * 4 + side_ * 2 + core_

    barrier = pltpu.get_barrier_semaphore()

    def greet(k, _):
        pl.semaphore_signal(barrier, inc=1, device_id={"rows": lax.rem(me + k, n)},
                            device_id_type=MESH)
        return 0

    lax.fori_loop(1, n, greet, 0)
    loads = [
        pltpu.make_async_copy(there, here, load_sem.at[index])
        for index, (there, here) in enumerate((
            (leaf_hbm, leaf_ref), (score_hbm, score_ref), (rel_hbm, rel_ref),
            (rank_hbm, rank_ref), (qlen_hbm, qlen_ref), (votes_hbm, votes_in),
            (elected_hbm, elected_ref), (fb_hbm, fb_ref)))
    ]
    for load in loads:
        load.start()
    for load in loads[:-1]:
        load.wait()

    pair_terms(chunks, leaf_ref, score_ref, rel_ref, rank_ref, qlen_ref, votes_in, packed_ref,
               stack_ref, grad_ref, hess_ref, leaves)

    lanes = lax.broadcasted_iota(jnp.int32, (leaves, features), 1)
    for e in range(picked):
        hot_ref[e * leaves:(e + 1) * leaves, :] = jnp.where(
            elected_ref[:, e:e + 1] == lanes, 1.0, 0.0).astype(BF16)
    loads[-1].wait()
    bins = fb_ref[...].astype(F32).astype(BF16)
    all_ref[...] = lax.dot_general(hot_ref[...], bins, NN, preferred_element_type=F32)

    sub = lax.broadcasted_iota(jnp.int32, (leaves, LANES), 0)
    own = [leaf_ref[c:c + 1, :] == sub for c in range(chunks)]
    grad, hess, leaf = grad_ref[...], hess_ref[...], leaf_ref[...].astype(F32)
    for i in range(n):
        for turn in range(turns):
            e = slot_of(i, turn, n)
            if e < picked:
                for c in range(chunks):
                    block = all_ref[e * leaves:(e + 1) * leaves, c * LANES:(c + 1) * LANES]
                    send_ref[i, turn * chunks + c:turn * chunks + c + 1, :] = jnp.sum(
                        jnp.where(own[c], block, 0.0), axis=0, keepdims=True)
            else:
                send_ref[i, turn * chunks:(turn + 1) * chunks, :] = jnp.zeros((chunks, LANES), F32)
        send_ref[i, base:base + chunks, :] = grad
        send_ref[i, base + chunks:base + 2 * chunks, :] = hess
        send_ref[i, base + 2 * chunks:base + 3 * chunks, :] = leaf
        rest = send_ref.shape[1] - base - 3 * chunks
        if rest:
            send_ref[i, base + 3 * chunks:, :] = jnp.zeros((rest, LANES), F32)

    pl.semaphore_wait(barrier, n - 1)

    def votes_copy(k):
        return pltpu.make_async_remote_copy(
            src_ref=packed_ref, dst_ref=votes_ref.at[me], send_sem=vs.at[k], recv_sem=vr.at[k],
            device_id={"rows": lax.rem(me + k, n)}, device_id_type=MESH)

    def docs_copy(k):
        there = lax.rem(me + k, n)
        return pltpu.make_async_remote_copy(
            src_ref=send_ref.at[there], dst_ref=docs_ref.at[me], send_sem=ds.at[k],
            recv_sem=dr.at[k], device_id={"rows": there}, device_id_type=MESH)

    def start_votes(k, _):
        votes_copy(k).start()
        return 0

    def start_docs(k, _):
        docs_copy(k).start()
        return 0

    lax.fori_loop(1, n, start_docs, 0)
    lax.fori_loop(1, n, start_votes, 0)
    votes_ref[me] = packed_ref[...]
    docs_ref[me] = send_ref[me]

    def wait_docs(k, _):
        docs_copy(k).wait()
        return 0

    lax.fori_loop(1, n, wait_docs, 0)
    subf = sub.astype(F32)

    def weigh(p, _):
        for c in range(chunks):
            own = docs_ref[p, base + 2 * chunks + c:base + 2 * chunks + c + 1, :] == subf
            for which in range(2):
                at_row = base + which * chunks + c
                left = docs_ref[p, at_row:at_row + 1, :]
                for term in range(TERMS):
                    piece = left.astype(BF16).astype(F32)
                    left = left - piece
                    at_weight = (term * 2 + which) * leaves
                    weight_ref[p, at_weight:at_weight + leaves, c * LANES:(c + 1) * LANES] = (
                        jnp.where(own, piece, 0.0).astype(BF16))
        return 0

    lax.fori_loop(0, n, weigh, 0)
    steps = [lax.broadcasted_iota(jnp.int32, (SUB, LANES), 0).astype(F32).astype(BF16)
             + jnp.asarray(first, BF16) for first in range(0, B, SUB)]
    one, zero = jnp.ones((SUB, LANES), BF16), jnp.zeros((SUB, LANES), BF16)

    def exists(owner, turn):
        return slot_of(owner, turn, n) < picked

    def tile_copy(slot, sems, rsems, index, there):
        return pltpu.make_async_remote_copy(
            src_ref=out_ref.at[slot], dst_ref=out_ref.at[slot], send_sem=sems.at[index],
            recv_sem=rsems.at[index], device_id={"rows": there}, device_id_type=MESH)

    def line_copy(k, turn):
        return tile_copy(slot_of(me, turn, n), zs, zr, k * turns + turn,
                         device(lax.rem(line + k, lines), side, core))

    def side_copy(line_, side_, turn):
        return tile_copy(slot_of(device(line_, side_, core), turn, n), ys, yr,
                         line_ * turns + turn, device(line, 1 - side, core))

    def core_copy(line_, side_, core_, turn):
        return tile_copy(slot_of(device(line_, side_, core_), turn, n), ss, sr,
                         (line_ * 2 + side_) * turns + turn, device(line, side, 1 - core))

    def save(owner, turn):
        slot = slot_of(owner, turn, n)
        return pltpu.make_async_copy(out_ref.at[slot], gain_hbm.at[slot], save_sem.at[slot])

    def guarded(owner, turn, action):
        @pl.when(exists(owner, turn))
        def _():
            action()

    for turn in range(turns):
        def work(turn=turn):
            def add(p, total):
                tall = []
                for c in range(chunks):
                    row = docs_ref[p, turn * chunks + c:turn * chunks + c + 1, :]
                    row = jnp.broadcast_to(row, (SUB, LANES)).astype(BF16)
                    tall.append(jnp.concatenate(
                        [jnp.where(row <= step, one, zero) for step in steps], axis=0))
                return total + lax.dot_general(
                    jnp.concatenate(tall, axis=1), weight_ref[p], NT, preferred_element_type=F32)

            total = lax.fori_loop(
                0, n, add, jnp.zeros((B, TERMS * 2 * leaves), F32), unroll=UNROLL).T
            both = total[:2 * leaves]
            for term in range(1, TERMS):
                both += total[term * 2 * leaves:(term + 1) * 2 * leaves]
            pg, ph = both[:leaves], both[leaves:]
            wg, wh = pg[:, B - 1:], ph[:, B - 1:]
            og, oh = wg - pg, wh - ph
            out_ref[slot_of(me, turn, n)] = (
                pg * pg / (ph + ridge_weight) + og * og / (oh + ridge_weight)
                - wg * wg / (wh + ridge_weight))

        def begin(turn=turn):
            side_copy(line, side, turn).start()
            for k in range(1, lines):
                line_copy(k, turn).start()
            core_copy(line, side, core, turn).start()
            save(me, turn).start()

        guarded(me, turn, work)
        guarded(me, turn, begin)

    def wait_votes(k, _):
        votes_copy(k).wait()
        return 0

    lax.fori_loop(1, n, wait_votes, 0)
    groups = leaves // 8
    pitch = LANES // groups
    numbers = lax.broadcasted_iota(jnp.int32, (8, features), 1)

    def count(p, totals):
        tile = votes_ref[p]
        grown = []
        for g in range(groups):
            total = totals[g]
            for k in range(votes_each):
                total += jnp.where(tile[:, g * pitch + k:g * pitch + k + 1] == numbers, 1, 0)
            grown.append(total)
        return tuple(grown)

    totals = lax.fori_loop(0, n, count, (jnp.zeros((8, features), jnp.int32),) * groups)
    for g in range(groups):
        count_ref[g * 8:(g + 1) * 8, :] = totals[g]

    for turn in range(turns):
        for k in range(1, lines):
            def pass_on(turn=turn, k=k):
                source = lax.rem(line + lines - k, lines)
                tile_copy(slot_of(device(source, side, core), turn, n), zs, zr, k * turns + turn,
                          device(lax.rem(line + k, lines), side, core)).wait_recv()
                side_copy(source, side, turn).start()
                core_copy(source, side, core, turn).start()
                save(device(source, side, core), turn).start()

            guarded(device(lax.rem(line + lines - k, lines), side, core), turn, pass_on)

    for turn in range(turns):
        for k in range(lines):
            def cross(turn=turn, k=k):
                source = lax.rem(line + lines - k, lines)
                side_copy(source, 1 - side, turn).wait_recv()
                core_copy(source, 1 - side, core, turn).start()
                save(device(source, 1 - side, core), turn).start()

            guarded(device(lax.rem(line + lines - k, lines), 1 - side, core), turn, cross)

    for turn in range(turns):
        for line_ in range(lines):
            for side_ in range(2):
                def last(turn=turn, line_=line_, side_=side_):
                    core_copy(line_, side_, 1 - core, turn).wait_recv()
                    save(device(line_, side_, 1 - core), turn).start()

                guarded(device(line_, side_, 1 - core), turn, last)
                guarded(device(line_, side_, core), turn,
                        lambda: core_copy(line_, side_, core, turn).wait_send())
            guarded(device(line_, side, core), turn,
                    lambda: side_copy(line_, side, turn).wait_send())
        for k in range(1, lines):
            guarded(me, turn, lambda: line_copy(k, turn).wait_send())
        for owner in range(n):
            if slot_of(owner, turn, n) < picked:
                save(owner, turn).wait()


def finish(grad_in, hess_in, count_in, gathered, grad_ref, hess_ref, count_ref, out_ref):
    grad_ref[...] = grad_in[...]
    hess_ref[...] = hess_in[...]
    count_ref[...] = count_in[...]
    out_ref[...] = jnp.swapaxes(gathered[...], 0, 1)


def on_device(n, feature_bin, doc_leaf, current_score, relevance, doc_rank, query_length,
              feature_votes, elected):
    docs, features = feature_bin.shape
    leaves, picked = elected.shape
    each = feature_votes.shape[2]
    turns = -(-picked // n)
    chunks = docs // LANES
    rows = -(-(turns + 3) * chunks // 8) * 8
    chips = n // 2
    lines = chips // 2

    def lay(a):
        return a.reshape(chunks, LANES)

    dma = pltpu.SemaphoreType.DMA
    gradient, hessian, vote_count, gathered = pl.pallas_call(
        functools.partial(kernel, n, turns),
        out_shape=(
            jax.ShapeDtypeStruct((chunks, LANES), F32),
            jax.ShapeDtypeStruct((chunks, LANES), F32),
            jax.ShapeDtypeStruct((leaves, features), jnp.int32),
            jax.ShapeDtypeStruct((picked, leaves, B), F32),
        ),
        in_specs=[pl.BlockSpec(memory_space=pltpu.HBM)] * 8,
        out_specs=(VMEM,) * 3 + (pl.BlockSpec(memory_space=pltpu.HBM),),
        scratch_shapes=[
            pltpu.VMEM((features, docs), jnp.int32),
            pltpu.VMEM((chunks, LANES), jnp.int32),
            pltpu.VMEM((chunks, LANES), F32),
            pltpu.VMEM((chunks, LANES), jnp.int32),
            pltpu.VMEM((chunks, LANES), jnp.int32),
            pltpu.SMEM(query_length.shape, jnp.int32),
            pltpu.VMEM((leaves, picked), jnp.int32),
            pltpu.VMEM((each, 1, leaves), jnp.int32),
            pltpu.VMEM((picked * leaves, features), BF16),
            pltpu.VMEM((LANES, LANES), F32),
            pltpu.VMEM((picked * leaves, docs), F32),
            pltpu.VMEM((8, LANES), jnp.int32),
            pltpu.VMEM((n, rows, LANES), F32),
            pltpu.VMEM((n, 8, LANES), jnp.int32),
            pltpu.VMEM((n, rows, LANES), F32),
            pltpu.VMEM((n, TERMS * 2 * leaves, docs), BF16),
            pltpu.VMEM((picked, leaves, B), F32),
            dma((8,)),
            dma((picked,)),
            dma((n,)), dma((n,)), dma((n,)), dma((n,)),
            dma((lines * turns,)), dma((lines * turns,)),
            dma((lines * turns,)), dma((lines * turns,)),
            dma((chips * turns,)), dma((chips * turns,)),
        ],
        compiler_params=pltpu.CompilerParams(
            collective_id=0, has_side_effects=True, vmem_limit_bytes=63 * 2**20),
        name="round",
    )(feature_bin.T, lay(doc_leaf), lay(current_score), lay(relevance), lay(doc_rank),
      query_length, elected, jnp.transpose(feature_votes, (2, 0, 1)))
    step = 8
    gradient, hessian, vote_count, split_gain = pl.pallas_call(
        finish,
        grid=(leaves // step,),
        out_shape=(
            jax.ShapeDtypeStruct((chunks, LANES), F32),
            jax.ShapeDtypeStruct((chunks, LANES), F32),
            jax.ShapeDtypeStruct((leaves, features), jnp.int32),
            jax.ShapeDtypeStruct((leaves, picked, B), F32),
        ),
        in_specs=[
            pl.BlockSpec((chunks, LANES), lambda i: (0, 0)),
            pl.BlockSpec((chunks, LANES), lambda i: (0, 0)),
            pl.BlockSpec((step, features), lambda i: (i, 0)),
            pl.BlockSpec((picked, step, B), lambda i: (0, i, 0)),
        ],
        out_specs=(
            pl.BlockSpec((chunks, LANES), lambda i: (0, 0)),
            pl.BlockSpec((chunks, LANES), lambda i: (0, 0)),
            pl.BlockSpec((step, features), lambda i: (i, 0)),
            pl.BlockSpec((step, picked, B), lambda i: (i, 0, 0)),
        ),
        compiler_params=pltpu.CompilerParams(vmem_limit_bytes=63 * 2**20),
        name="finish",
    )(gradient, hessian, vote_count, gathered)
    return gradient.reshape(-1), hessian.reshape(-1), vote_count, split_gain


def solution(mesh):
    n = mesh.shape["rows"]
    return jax.shard_map(
        functools.partial(on_device, n),
        mesh=mesh,
        in_specs=(
            P(("parts", "rows"), None),
            P(("parts", "rows")),
            P(("parts", "rows")),
            P(("parts", "rows")),
            P(("parts", "rows")),
            P(("parts", "rows")),
            P(("parts", "rows"), None, None),
            P("parts", None),
        ),
        out_specs=(
            P(("parts", "rows")),
            P(("parts", "rows")),
            P("parts", None),
            P("parts", None, None),
        ),
        check_vma=False,
    )
```

```python
import functools
import math

import jax
import jax.numpy as jnp
from jax import lax
from jax.experimental import pallas as pl
from jax.experimental.pallas import tpu as pltpu
from jax.sharding import PartitionSpec as P

B = 256
QMAX = 256
LANES = 128
SUB = 16
TERMS = 2
UNROLL = 16

ridge_weight = 1.0
F32 = jnp.float32
BF16 = jnp.bfloat16
NT = (((1,), (1,)), ((), ()))
NN = (((1,), (0,)), ((), ()))
VMEM = pl.BlockSpec(memory_space=pltpu.VMEM)
MESH = pl.DeviceIdType.MESH


def slot_of(owner, turn, n):
    return turn * n + (owner % 2) * (n // 2) + owner // 2


def pair_terms(chunks, leaf_ref, score_ref, rel_ref, rank_ref, qlen_ref, votes_ref, packed_ref,
               stack_ref, grad_ref, hess_ref, leaves):
    per_query = QMAX // LANES
    each = votes_ref.shape[0]
    rel = rel_ref[...].astype(F32)
    gain = jnp.exp2(rel) - 1.0
    disc = math.log(2.0) / jnp.log(rank_ref[...].astype(F32) + 2.0)
    row = lax.broadcasted_iota(jnp.int32, (chunks, LANES), 0)
    slot = (row % per_query) * LANES + lax.broadcasted_iota(jnp.int32, (chunks, LANES), 1)
    length = jnp.zeros((chunks, LANES), jnp.int32)
    for q in range(chunks // per_query):
        length = jnp.where(row // per_query == q, qlen_ref[q], length)
    live = slot < length
    livef = jnp.where(live, 1.0, 0.0)
    key = rel * float(QMAX) + (QMAX - 1 - slot).astype(F32)
    score = score_ref[...]
    stack_ref[...] = jnp.zeros(stack_ref.shape, F32)
    items = (score, gain, disc, jnp.where(live, key, -1.0), livef)
    for index, item in enumerate(items):
        stack_ref[index * chunks:(index + 1) * chunks, :] = item
    first = len(items) * chunks
    for k in range(each):
        stack_ref[first + k:first + k + 1, 0:leaves] = votes_ref[k].astype(F32)
    turned = stack_ref[...].T

    groups = leaves // 8
    pitch = LANES // groups
    packed_ref[...] = jnp.full(packed_ref.shape, -1, jnp.int32)
    for g in range(groups):
        packed_ref[:, g * pitch:g * pitch + each] = turned[
            g * 8:(g + 1) * 8, first:first + each].astype(jnp.int32)

    def column(index, c):
        return turned[:, index * chunks + c:index * chunks + c + 1]

    for q in range(chunks // per_query):
        mine = range(q * per_query, (q + 1) * per_query)
        ideal = jnp.zeros((1, 1), F32)
        sums = []
        for j in mine:
            srow, grow, drow, krow = score[j:j + 1], gain[j:j + 1], disc[j:j + 1], key[j:j + 1]
            place = jnp.zeros((1, LANES), F32)
            push = jnp.zeros((1, LANES), F32)
            curve = jnp.zeros((1, LANES), F32)
            for i in mine:
                place += jnp.sum(jnp.where(column(3, i) > krow, 1.0, 0.0), axis=0, keepdims=True)
                apart = column(0, i) - srow
                step = column(1, i) - grow
                chance = 1.0 / (1.0 + jnp.exp(jnp.where(step > 0.0, apart, -apart)))
                part = chance * jnp.abs(column(2, i) - drow) * column(4, i)
                signed = part * step
                push += jnp.sum(signed, axis=0, keepdims=True)
                curve += jnp.sum(jnp.abs(signed) * (1.0 - chance), axis=0, keepdims=True)
            top = livef[j:j + 1] * grow * (math.log(2.0) / jnp.log(place + 2.0))
            ideal += jnp.sum(top, axis=1, keepdims=True)
            sums.append((push, curve))
        scaling = 1.0 / jnp.maximum(ideal, 1.0)
        for j, (push, curve) in zip(mine, sums):
            grad_ref[j:j + 1, :] = push * livef[j:j + 1] * scaling
            hess_ref[j:j + 1, :] = curve * livef[j:j + 1] * scaling


def kernel(n, turns, fb_hbm, leaf_hbm, score_hbm, rel_hbm, rank_hbm, qlen_hbm, elected_hbm,
           votes_hbm, grad_ref, hess_ref, count_ref, gain_hbm,
           fb_ref, leaf_ref, score_ref, rel_ref, rank_ref, qlen_ref, elected_ref, votes_in,
           hot_ref, stack_ref, all_ref, packed_ref, send_ref,
           votes_ref, docs_ref, weight_ref, out_ref, load_sem, save_sem, vs, vr, ds, dr, zs, zr, ys, yr, ss, sr):
    features, docs = fb_ref.shape
    leaves, picked = elected_ref.shape
    votes_each = votes_in.shape[0]
    chunks = docs // LANES
    base = turns * chunks
    chips = n // 2
    lines = chips // 2
    me = lax.axis_index("rows")
    core, side, line = me % 2, (me // 2) % 2, me // 4

    def device(line_, side_, core_):
        return line_ * 4 + side_ * 2 + core_

    barrier = pltpu.get_barrier_semaphore()

    def greet(k, _):
        pl.semaphore_signal(barrier, inc=1, device_id={"rows": lax.rem(me + k, n)},
                            device_id_type=MESH)
        return 0

    lax.fori_loop(1, n, greet, 0)
    loads = [
        pltpu.make_async_copy(there, here, load_sem.at[index])
        for index, (there, here) in enumerate((
            (leaf_hbm, leaf_ref), (score_hbm, score_ref), (rel_hbm, rel_ref),
            (rank_hbm, rank_ref), (qlen_hbm, qlen_ref), (votes_hbm, votes_in),
            (elected_hbm, elected_ref), (fb_hbm, fb_ref)))
    ]
    for load in loads:
        load.start()
    for load in loads[:-1]:
        load.wait()

    pair_terms(chunks, leaf_ref, score_ref, rel_ref, rank_ref, qlen_ref, votes_in, packed_ref,
               stack_ref, grad_ref, hess_ref, leaves)

    lanes = lax.broadcasted_iota(jnp.int32, (leaves, features), 1)
    for e in range(picked):
        hot_ref[e * leaves:(e + 1) * leaves, :] = jnp.where(
            elected_ref[:, e:e + 1] == lanes, 1.0, 0.0).astype(BF16)
    loads[-1].wait()
    bins = fb_ref[...].astype(F32).astype(BF16)
    all_ref[...] = lax.dot_general(hot_ref[...], bins, NN, preferred_element_type=F32)

    sub = lax.broadcasted_iota(jnp.int32, (leaves, LANES), 0)
    own = [leaf_ref[c:c + 1, :] == sub for c in range(chunks)]
    grad, hess, leaf = grad_ref[...], hess_ref[...], leaf_ref[...].astype(F32)
    for i in range(n):
        for turn in range(turns):
            e = slot_of(i, turn, n)
            if e < picked:
                for c in range(chunks):
                    block = all_ref[e * leaves:(e + 1) * leaves, c * LANES:(c + 1) * LANES]
                    send_ref[i, turn * chunks + c:turn * chunks + c + 1, :] = jnp.sum(
                        jnp.where(own[c], block, 0.0), axis=0, keepdims=True)
            else:
                send_ref[i, turn * chunks:(turn + 1) * chunks, :] = jnp.zeros((chunks, LANES), F32)
        send_ref[i, base:base + chunks, :] = grad
        send_ref[i, base + chunks:base + 2 * chunks, :] = hess
        send_ref[i, base + 2 * chunks:base + 3 * chunks, :] = leaf
        rest = send_ref.shape[1] - base - 3 * chunks
        if rest:
            send_ref[i, base + 3 * chunks:, :] = jnp.zeros((rest, LANES), F32)

    pl.semaphore_wait(barrier, n - 1)

    def votes_copy(k):
        return pltpu.make_async_remote_copy(
            src_ref=packed_ref, dst_ref=votes_ref.at[me], send_sem=vs.at[k], recv_sem=vr.at[k],
            device_id={"rows": lax.rem(me + k, n)}, device_id_type=MESH)

    def docs_copy(k):
        there = lax.rem(me + k, n)
        return pltpu.make_async_remote_copy(
            src_ref=send_ref.at[there], dst_ref=docs_ref.at[me], send_sem=ds.at[k],
            recv_sem=dr.at[k], device_id={"rows": there}, device_id_type=MESH)

    def start_votes(k, _):
        votes_copy(k).start()
        return 0

    def start_docs(k, _):
        docs_copy(k).start()
        return 0

    lax.fori_loop(1, n, start_docs, 0)
    votes_ref[me] = packed_ref[...]
    docs_ref[me] = send_ref[me]

    def wait_docs(k, _):
        docs_copy(k).wait()
        return 0

    lax.fori_loop(1, n, wait_docs, 0)
    lax.fori_loop(1, n, start_votes, 0)
    subf = sub.astype(F32)

    def weigh(p, _):
        for c in range(chunks):
            own = docs_ref[p, base + 2 * chunks + c:base + 2 * chunks + c + 1, :] == subf
            for which in range(2):
                at_row = base + which * chunks + c
                left = docs_ref[p, at_row:at_row + 1, :]
                for term in range(TERMS):
                    piece = left.astype(BF16).astype(F32)
                    left = left - piece
                    at_weight = (term * 2 + which) * leaves
                    weight_ref[p, at_weight:at_weight + leaves, c * LANES:(c + 1) * LANES] = (
                        jnp.where(own, piece, 0.0).astype(BF16))
        return 0

    lax.fori_loop(0, n, weigh, 0)
    steps = [lax.broadcasted_iota(jnp.int32, (SUB, LANES), 0).astype(F32).astype(BF16)
             + jnp.asarray(first, BF16) for first in range(0, B, SUB)]
    one, zero = jnp.ones((SUB, LANES), BF16), jnp.zeros((SUB, LANES), BF16)

    def exists(owner, turn):
        return slot_of(owner, turn, n) < picked

    def tile_copy(slot, sems, rsems, index, there):
        return pltpu.make_async_remote_copy(
            src_ref=out_ref.at[slot], dst_ref=out_ref.at[slot], send_sem=sems.at[index],
            recv_sem=rsems.at[index], device_id={"rows": there}, device_id_type=MESH)

    def line_copy(k, turn):
        return tile_copy(slot_of(me, turn, n), zs, zr, k * turns + turn,
                         device(lax.rem(line + k, lines), side, core))

    def side_copy(line_, side_, turn):
        return tile_copy(slot_of(device(line_, side_, core), turn, n), ys, yr,
                         line_ * turns + turn, device(line, 1 - side, core))

    def core_copy(line_, side_, core_, turn):
        return tile_copy(slot_of(device(line_, side_, core_), turn, n), ss, sr,
                         (line_ * 2 + side_) * turns + turn, device(line, side, 1 - core))

    def save(owner, turn):
        slot = slot_of(owner, turn, n)
        return pltpu.make_async_copy(out_ref.at[slot], gain_hbm.at[slot], save_sem.at[slot])

    def guarded(owner, turn, action):
        @pl.when(exists(owner, turn))
        def _():
            action()

    for turn in range(turns):
        def work(turn=turn):
            def add(p, total):
                tall = []
                for c in range(chunks):
                    row = docs_ref[p, turn * chunks + c:turn * chunks + c + 1, :]
                    row = jnp.broadcast_to(row, (SUB, LANES)).astype(BF16)
                    tall.append(jnp.concatenate(
                        [jnp.where(row <= step, one, zero) for step in steps], axis=0))
                return total + lax.dot_general(
                    jnp.concatenate(tall, axis=1), weight_ref[p], NT, preferred_element_type=F32)

            total = lax.fori_loop(
                0, n, add, jnp.zeros((B, TERMS * 2 * leaves), F32), unroll=UNROLL).T
            both = total[:2 * leaves]
            for term in range(1, TERMS):
                both += total[term * 2 * leaves:(term + 1) * 2 * leaves]
            pg, ph = both[:leaves], both[leaves:]
            wg, wh = pg[:, B - 1:], ph[:, B - 1:]
            og, oh = wg - pg, wh - ph
            out_ref[slot_of(me, turn, n)] = (
                pg * pg / (ph + ridge_weight) + og * og / (oh + ridge_weight)
                - wg * wg / (wh + ridge_weight))

        def begin(turn=turn):
            side_copy(line, side, turn).start()
            for k in range(1, lines):
                line_copy(k, turn).start()
            core_copy(line, side, core, turn).start()
            save(me, turn).start()

        guarded(me, turn, work)
        guarded(me, turn, begin)

    def wait_votes(k, _):
        votes_copy(k).wait()
        return 0

    groups = leaves // 8
    pitch = LANES // groups
    numbers = lax.broadcasted_iota(jnp.int32, (8, features), 1)

    def count(p, totals):
        tile = votes_ref[p]
        grown = []
        for g in range(groups):
            total = totals[g]
            for k in range(votes_each):
                total += jnp.where(tile[:, g * pitch + k:g * pitch + k + 1] == numbers, 1, 0)
            grown.append(total)
        return tuple(grown)

    shares = turns + 1

    def count_share(share):
        low, high = share * n // shares, (share + 1) * n // shares
        if share == 0:
            lax.fori_loop(1, n, wait_votes, 0)
            start = (jnp.zeros((8, features), jnp.int32),) * groups
        else:
            start = tuple(count_ref[g * 8:(g + 1) * 8, :] for g in range(groups))
        totals = lax.fori_loop(low, high, count, start)
        for g in range(groups):
            count_ref[g * 8:(g + 1) * 8, :] = totals[g]

    for turn in range(turns):
        count_share(turn)
        for k in range(1, lines):
            def pass_on(turn=turn, k=k):
                source = lax.rem(line + lines - k, lines)
                tile_copy(slot_of(device(source, side, core), turn, n), zs, zr, k * turns + turn,
                          device(lax.rem(line + k, lines), side, core)).wait_recv()
                side_copy(source, side, turn).start()
                core_copy(source, side, core, turn).start()
                save(device(source, side, core), turn).start()

            guarded(device(lax.rem(line + lines - k, lines), side, core), turn, pass_on)

    count_share(turns)
    for turn in range(turns):
        for k in range(lines):
            def cross(turn=turn, k=k):
                source = lax.rem(line + lines - k, lines)
                side_copy(source, 1 - side, turn).wait_recv()
                core_copy(source, 1 - side, core, turn).start()
                save(device(source, 1 - side, core), turn).start()

            guarded(device(lax.rem(line + lines - k, lines), 1 - side, core), turn, cross)

    for turn in range(turns):
        for line_ in range(lines):
            for side_ in range(2):
                def last(turn=turn, line_=line_, side_=side_):
                    core_copy(line_, side_, 1 - core, turn).wait_recv()
                    save(device(line_, side_, 1 - core), turn).start()

                guarded(device(line_, side_, 1 - core), turn, last)
                guarded(device(line_, side_, core), turn,
                        lambda: core_copy(line_, side_, core, turn).wait_send())
            guarded(device(line_, side, core), turn,
                    lambda: side_copy(line_, side, turn).wait_send())
        for k in range(1, lines):
            guarded(me, turn, lambda: line_copy(k, turn).wait_send())
        for owner in range(n):
            if slot_of(owner, turn, n) < picked:
                save(owner, turn).wait()


def finish(grad_in, hess_in, count_in, gathered, grad_ref, hess_ref, count_ref, out_ref):
    grad_ref[...] = grad_in[...]
    hess_ref[...] = hess_in[...]
    count_ref[...] = count_in[...]
    out_ref[...] = jnp.swapaxes(gathered[...], 0, 1)


def on_device(n, feature_bin, doc_leaf, current_score, relevance, doc_rank, query_length,
              feature_votes, elected):
    docs, features = feature_bin.shape
    leaves, picked = elected.shape
    each = feature_votes.shape[2]
    turns = -(-picked // n)
    chunks = docs // LANES
    rows = -(-(turns + 3) * chunks // 8) * 8
    chips = n // 2
    lines = chips // 2

    def lay(a):
        return a.reshape(chunks, LANES)

    dma = pltpu.SemaphoreType.DMA
    gradient, hessian, vote_count, gathered = pl.pallas_call(
        functools.partial(kernel, n, turns),
        out_shape=(
            jax.ShapeDtypeStruct((chunks, LANES), F32),
            jax.ShapeDtypeStruct((chunks, LANES), F32),
            jax.ShapeDtypeStruct((leaves, features), jnp.int32),
            jax.ShapeDtypeStruct((picked, leaves, B), F32),
        ),
        in_specs=[pl.BlockSpec(memory_space=pltpu.HBM)] * 8,
        out_specs=(VMEM,) * 3 + (pl.BlockSpec(memory_space=pltpu.HBM),),
        scratch_shapes=[
            pltpu.VMEM((features, docs), jnp.int32),
            pltpu.VMEM((chunks, LANES), jnp.int32),
            pltpu.VMEM((chunks, LANES), F32),
            pltpu.VMEM((chunks, LANES), jnp.int32),
            pltpu.VMEM((chunks, LANES), jnp.int32),
            pltpu.SMEM(query_length.shape, jnp.int32),
            pltpu.VMEM((leaves, picked), jnp.int32),
            pltpu.VMEM((each, 1, leaves), jnp.int32),
            pltpu.VMEM((picked * leaves, features), BF16),
            pltpu.VMEM((LANES, LANES), F32),
            pltpu.VMEM((picked * leaves, docs), F32),
            pltpu.VMEM((8, LANES), jnp.int32),
            pltpu.VMEM((n, rows, LANES), F32),
            pltpu.VMEM((n, 8, LANES), jnp.int32),
            pltpu.VMEM((n, rows, LANES), F32),
            pltpu.VMEM((n, TERMS * 2 * leaves, docs), BF16),
            pltpu.VMEM((picked, leaves, B), F32),
            dma((8,)),
            dma((picked,)),
            dma((n,)), dma((n,)), dma((n,)), dma((n,)),
            dma((lines * turns,)), dma((lines * turns,)),
            dma((lines * turns,)), dma((lines * turns,)),
            dma((chips * turns,)), dma((chips * turns,)),
        ],
        compiler_params=pltpu.CompilerParams(
            collective_id=0, has_side_effects=True, vmem_limit_bytes=63 * 2**20),
        name="round",
    )(feature_bin.T, lay(doc_leaf), lay(current_score), lay(relevance), lay(doc_rank),
      query_length, elected, jnp.transpose(feature_votes, (2, 0, 1)))
    step = 16
    gradient, hessian, vote_count, split_gain = pl.pallas_call(
        finish,
        grid=(leaves // step,),
        out_shape=(
            jax.ShapeDtypeStruct((chunks, LANES), F32),
            jax.ShapeDtypeStruct((chunks, LANES), F32),
            jax.ShapeDtypeStruct((leaves, features), jnp.int32),
            jax.ShapeDtypeStruct((leaves, picked, B), F32),
        ),
        in_specs=[
            pl.BlockSpec((chunks, LANES), lambda i: (0, 0)),
            pl.BlockSpec((chunks, LANES), lambda i: (0, 0)),
            pl.BlockSpec((step, features), lambda i: (i, 0)),
            pl.BlockSpec((picked, step, B), lambda i: (0, i, 0)),
        ],
        out_specs=(
            pl.BlockSpec((chunks, LANES), lambda i: (0, 0)),
            pl.BlockSpec((chunks, LANES), lambda i: (0, 0)),
            pl.BlockSpec((step, features), lambda i: (i, 0)),
            pl.BlockSpec((step, picked, B), lambda i: (i, 0, 0)),
        ),
        compiler_params=pltpu.CompilerParams(vmem_limit_bytes=63 * 2**20),
        name="finish",
    )(gradient, hessian, vote_count, gathered)
    return gradient.reshape(-1), hessian.reshape(-1), vote_count, split_gain


def solution(mesh):
    n = mesh.shape["rows"]
    return jax.shard_map(
        functools.partial(on_device, n),
        mesh=mesh,
        in_specs=(
            P(("parts", "rows"), None),
            P(("parts", "rows")),
            P(("parts", "rows")),
            P(("parts", "rows")),
            P(("parts", "rows")),
            P(("parts", "rows")),
            P(("parts", "rows"), None, None),
            P("parts", None),
        ),
        out_specs=(
            P(("parts", "rows")),
            P(("parts", "rows")),
            P("parts", None),
            P("parts", None, None),
        ),
        check_vma=False,
    )
```
